128 devices in a mesh: rep: 8 (over z, y_lo), fsdp: 16 (over y_hi, x, core).
Axes of the slice: x: 4, y: 4 (y_hi: 2, y_lo: 2; y = y_hi * 2 + y_lo), z: 4, core: 2. Of those that a mesh axis runs over, the one named last changes fastest.
Arguments:
- tokens: bfloat16 [65536, 2048], P(('rep', 'fsdp')), may hold values from -6 to 6
- norm_gain: float32 [2048], replicated, may hold values from 0.5 to 1.5
- outer_params: float32 [2, 2048, 4096], P(None, 'fsdp'), may hold values from -6 to 6
- momentum: float32 [2, 2048, 4096], P(None, 'fsdp'), may hold values from -6 to 6
- deltas: bfloat16 [8, 2, 2048, 4096], P('rep', None, 'fsdp'), may hold values from -6 to 6
Outputs:
- new_params: float32 [2, 2048, 4096], P(None, 'fsdp')
- new_momentum: float32 [2, 2048, 4096], P(None, 'fsdp')
- hidden: bfloat16 [65536, 4096], P(('rep', 'fsdp'))
The draws below stay inside these ranges and needn't reach their ends.
All inputs are finite; a program needn't handle non-finite values.
Results may differ from the reference program's by a relative error of at most 0.01.
Values may be sent and summed in bfloat16 or wider, within the bound.
A program may use at most 192 MiB of HBM per device.

```python
import math
import jax
import jax.numpy as jnp
from jax import lax

D = 2048
FF = 4096
TOKENS = 65536
N_REP = 8


def block_levels(stream_key, shape, split, least, largest):
    def one(position, blocks):
        heights = jax.random.uniform(jax.random.fold_in(jax.random.fold_in(stream_key, 6), position), (blocks,), jnp.float32, least / len(split), largest / len(split))
        return jnp.repeat(jnp.exp(heights), shape[position] // blocks).reshape((-1,) + (1,) * (len(shape) - position - 1))

    loudness = one(*split[0])
    for cut in split[1:]:
        loudness = loudness * one(*cut)
    return loudness


def normal_values(stream_key, dims, deviation, most, pieces=(), held_as=jnp.bfloat16):
    values = jax.random.normal(stream_key, dims, jnp.float32) * deviation
    if len(pieces) > 0:
        values = block_levels(stream_key, dims, pieces, -0.22, 0.18) * values
    return jnp.clip(values, min=-most, max=most).astype(held_as)


def setup_inputs(seed: int = 0) -> dict:
    key_list = jax.random.split(jax.random.key(seed), 6)
    return {
        "tokens": normal_values(key_list[0], (TOKENS, D), 1.0, 6.0, ((0, 128),)),
        "norm_gain": jnp.clip(1.0 + 0.1 * jax.random.normal(key_list[1], (D,), jnp.float32), 0.5, 1.5),
        "outer_params": normal_values(key_list[2], (2, D, FF), 1.0, 6.0, ((1, 16),), jnp.float32),
        "momentum": normal_values(key_list[3], (2, D, FF), 0.5, 6.0, ((1, 16),), jnp.float32),
        "deltas": normal_values(key_list[4], (N_REP, 2, D, FF), 0.5, 6.0, ((0, 8), (2, 16))),
    }


EPS = 1e-05
MU = 0.9
RATE = 0.7

def reference(tokens, norm_gain, outer_params, momentum, deltas):
    total = jnp.zeros(outer_params.shape, jnp.float32)
    for group in range(N_REP):
        total = total + deltas[group].astype(jnp.float32)
    outer_grad = total / N_REP
    new_momentum = MU * momentum + outer_grad
    new_params = outer_params - RATE * (outer_grad + MU * new_momentum)
    weights = new_params.astype(jnp.bfloat16)
    values = tokens.astype(jnp.float32)
    scale_rows = lax.rsqrt(lax.optimization_barrier(jnp.mean(values * values, axis=-1, keepdims=True)) + EPS)
    normed = (values * scale_rows * norm_gain).astype(jnp.bfloat16)
    factor = 1.0 / math.sqrt(D)
    gate = jnp.dot(normed, weights[0], preferred_element_type=jnp.float32) * factor
    up = jnp.dot(normed, weights[1], preferred_element_type=jnp.float32) * factor
    hidden = (jax.nn.silu(gate) * up).astype(jnp.bfloat16)
    return (new_params, new_momentum, hidden)
```

```python
import functools
import math

import jax
import jax.numpy as jnp
from jax import lax
from jax.experimental import pallas as pl
from jax.experimental.pallas import tpu as pltpu
from jax.sharding import PartitionSpec as P

EPS = 1e-05
MU = 0.9
RATE = 0.7
MESH = pl.DeviceIdType.MESH

CHUNKS = 8
GROUPS = 8
XS = 4


def kernel(
    tok_ref, gain_ref, p_ref, m_ref, d_ref,
    sums_ref, hid_ref,
    dl, rs, sm, pb, mb, w, stg, tk, nt, ob,
    ld_d, ld_p, ld_m, ld_t,
    rs_s, rs_r, sm_s, sm_r, d2_s, d2_r, nt_s, nt_r,
    yo_s, yo_r, x_s, x_r, f_s, f_r, o_l, o_s, o_r, so_s,
):
    n = CHUNKS
    rows = dl.shape[3]
    wc = dl.shape[4]
    half = n * wc
    piece = rows // GROUPS
    tokens = tk.shape[0]
    width = tk.shape[1]

    rep = lax.axis_index("rep")
    fs = lax.axis_index("fsdp")
    core = lax.rem(fs, 2)
    other = 1 - core
    chip = fs // 2
    x = lax.rem(chip, XS)
    yh = chip // XS
    yl = lax.rem(rep, 2)
    z = rep // 2
    x_up = lax.rem(x + 1, XS)
    x_dn = lax.rem(x + XS - 1, XS)

    def fsdp_of(yh_, x_, core_):
        return (yh_ * XS + x_) * 2 + core_

    partner = (rep, fsdp_of(yh, x, other))
    across = (z * 2 + 1 - yl, fsdp_of(1 - yh, x, core))
    up = (rep, fsdp_of(yh, x_up, core))
    down = (rep, fsdp_of(yh, x_dn, core))
    peers = [(lax.rem(rep + k, GROUPS), fs) for k in range(1, GROUPS)]

    def load(src, dst, sem, j, h):
        return pltpu.make_async_copy(
            src.at[:, :, pl.ds(pl.multiple_of(h * half + j * wc, wc), wc)],
            dst.at[j, h],
            sem.at[j, h],
        )

    def remote(src, dst, send, recv, device):
        return pltpu.make_async_remote_copy(
            src_ref=src, dst_ref=dst, send_sem=send, recv_sem=recv,
            device_id=device, device_id_type=MESH,
        )

    def rs_copy(j, k):
        rows_of = pl.multiple_of(peers[k][0] * piece, piece)
        return remote(
            dl.at[j, :, :, pl.ds(rows_of, piece), :], rs.at[j, k],
            rs_s.at[j, k], rs_r.at[j, k], peers[k],
        )

    def sm_copy(j, k):
        mine = pl.ds(pl.multiple_of(rep * piece, piece), piece)
        ref = sm.at[j, :, :, mine, :]
        return remote(ref, ref, sm_s.at[j, k], sm_r.at[j, k], peers[k])

    def d2_copy(j):
        at = pl.ds(pl.multiple_of(core * rows, rows), rows)
        return remote(
            stg.at[j], w.at[j, :, yh, x, at, :], d2_s.at[j], d2_r.at[j], partner
        )

    def yo_copy(j):
        ref = w.at[j, :, yh, x]
        return remote(ref, ref, yo_s.at[j], yo_r.at[j], across)

    def x_copy(j, k):
        ref = w.at[j, :, :, x]
        return remote(ref, ref, x_s.at[j, k], x_r.at[j, k], (up, down)[k])

    def f_copy(j, k):
        ref = w.at[j, :, :, (x_dn, x_up)[k], pl.ds(k * rows, rows), :]
        return remote(ref, ref, f_s.at[j, k], f_r.at[j, k], (up, down)[k])

    def nt_copy():
        ref = nt.at[pl.ds(pl.multiple_of(core * tokens, tokens), tokens), :]
        return remote(ref, ref, nt_s.at[0], nt_r.at[0], partner)

    def column(j):
        return pl.ds(pl.multiple_of(core * half + j * wc, wc), wc)

    def own_out(j):
        at = pl.ds(pl.multiple_of(core * tokens, tokens), tokens)
        return pltpu.make_async_copy(
            ob.at[j, at, :], hid_ref.at[:, column(j)], o_l.at[j]
        )

    def far_out(j):
        at = pl.ds(pl.multiple_of(other * tokens, tokens), tokens)
        return remote(
            ob.at[j, at, :], hid_ref.at[:, column(j)], o_s.at[j], o_r.at[j], partner
        )

    def sums_out(j, h):
        return pltpu.make_async_copy(
            sm.at[j, h],
            sums_ref.at[:, :, pl.ds(pl.multiple_of(h * half + j * wc, wc), wc)],
            so_s.at[j, h],
        )

    def both(fn):
        for h in range(2):
            fn(h)

    @pl.loop(0, n)
    def _(j):
        both(lambda h: load(d_ref, dl, ld_d, j, h).start())

    pltpu.make_async_copy(tok_ref, tk, ld_t.at[0]).start()

    @pl.loop(0, n)
    def _(j):
        both(lambda h: load(p_ref, pb, ld_p, j, h).start())
        both(lambda h: load(m_ref, mb, ld_m, j, h).start())

    barrier = pltpu.get_barrier_semaphore()
    friends = peers + [partner, across, up, down]
    for friend in friends:
        pl.semaphore_signal(barrier, inc=1, device_id=friend, device_id_type=MESH)
    pl.semaphore_wait(barrier, len(friends))

    def scatter(j):
        both(lambda h: load(d_ref, dl, ld_d, j, h).wait())
        for k in range(GROUPS - 1):
            rs_copy(j, k).start()

    for j in range(2):
        scatter(j)

    pltpu.make_async_copy(tok_ref, tk, ld_t.at[0]).wait()
    step = 32

    @pl.loop(0, tokens // step)
    def _(i):
        at = pl.multiple_of(i * step, step)
        values = tk[pl.ds(at, step), :].astype(jnp.float32)
        mean = jnp.sum(values * values, axis=1, keepdims=True) * (1.0 / width)
        scaled = values * lax.rsqrt(mean + EPS) * gain_ref[...]
        base = pl.multiple_of(core * tokens + at, step)
        nt[pl.ds(base, step), :] = scaled.astype(jnp.bfloat16)

    def add_up(j):
        for k in range(GROUPS - 1):
            rs_copy(j, k).wait_recv()
        mine = pl.ds(pl.multiple_of(rep * piece, piece), piece)
        for h in range(2):
            for q in range(2):
                total = dl[j, h, q, mine, :].astype(jnp.float32)
                for k in range(GROUPS - 1):
                    total = total + rs[j, k, h, q].astype(jnp.float32)
                sm[j, h, q, mine, :] = total.astype(jnp.bfloat16)

    def update(j):
        for k in range(GROUPS - 1):
            sm_copy(j, k).wait_recv()
        both(lambda h: load(p_ref, pb, ld_p, j, h).wait())
        both(lambda h: load(m_ref, mb, ld_m, j, h).wait())
        at = pl.ds(pl.multiple_of(core * rows, rows), rows)

        def weights(h, q):
            grad = sm[j, h, q].astype(jnp.float32) * (1.0 / GROUPS)
            moment = MU * mb[j, h, q] + grad
            fresh = pb[j, h, q] - RATE * (grad + MU * moment)
            return fresh.astype(jnp.bfloat16)

        for q in range(2):
            stg[j, q] = weights(other, q)
        for q in range(2):
            w[j, q, yh, x, at, :] = weights(core, q)
        both(lambda h: sums_out(j, h).start())

    factor = 1.0 / math.sqrt(width)
    tile = 256

    def project(j):
        @pl.loop(0, 2 * tokens // tile)
        def _(i):
            at = pl.ds(pl.multiple_of(i * tile, tile), tile)
            left = nt[at, :]
            gate = jnp.dot(
                left, w[j, 0].reshape(width, wc), preferred_element_type=jnp.float32
            ) * factor
            raised = jnp.dot(
                left, w[j, 1].reshape(width, wc), preferred_element_type=jnp.float32
            ) * factor
            ob[j, at, :] = (gate / (1.0 + jnp.exp(-gate)) * raised).astype(jnp.bfloat16)

    nt_copy().start()

    @pl.loop(0, n + 5)
    def _(t):
        def stage(lag, fn):
            j = t - lag

            @pl.when(jnp.logical_and(j >= 0, j < n))
            def _():
                fn(j)

        def stage_x(j):
            yo_copy(j).wait_recv()
            for k in range(2):
                x_copy(j, k).start()

        def stage_y(j):
            d2_copy(j).wait_recv()
            yo_copy(j).start()

        def stage_send_sums(j):
            for k in range(GROUPS - 1):
                sm_copy(j, k).start()

        def stage_forward(j):
            for k in range(2):
                x_copy(j, k).wait_recv()
                f_copy(j, k).start()

        def stage_project(j):
            for k in range(2):
                f_copy(j, k).wait_recv()

            @pl.when(j == 0)
            def _():
                nt_copy().wait_recv()

            project(j)
            own_out(j).start()
            far_out(j).start()

        stage(3, stage_x)
        stage(2, stage_y)
        stage(1, update)
        stage(0, add_up)
        stage(1, lambda j: d2_copy(j).start())
        stage(-2, scatter)
        stage(0, stage_send_sums)
        stage(4, stage_forward)
        stage(5, stage_project)

    nt_copy().wait_send()

    @pl.loop(0, n)
    def _(j):
        for k in range(GROUPS - 1):
            rs_copy(j, k).wait_send()
            sm_copy(j, k).wait_send()
        d2_copy(j).wait_send()
        yo_copy(j).wait_send()
        for k in range(2):
            x_copy(j, k).wait_send()
            f_copy(j, k).wait_send()
        both(lambda h: sums_out(j, h).wait())
        own_out(j).wait()
        far_out(j).wait_send()
        far_out(j).wait_recv()


def fused(tokens, gain, params, moment, deltas):
    count, width = tokens.shape
    _, rows, cols = params.shape
    n = CHUNKS
    wc = cols // (2 * n)
    piece = rows // GROUPS
    bf16, f32 = jnp.bfloat16, jnp.float32
    dma = pltpu.SemaphoreType.DMA
    any_spec = pl.BlockSpec(memory_space=pl.ANY)
    return pl.pallas_call(
        kernel,
        out_shape=(
            jax.ShapeDtypeStruct((2, rows, cols), bf16),
            jax.ShapeDtypeStruct((count, cols), bf16),
        ),
        in_specs=[any_spec, pl.BlockSpec(memory_space=pltpu.VMEM), any_spec, any_spec, any_spec],
        out_specs=(any_spec, any_spec),
        scratch_shapes=[
            pltpu.VMEM((n, 2, 2, rows, wc), bf16),
            pltpu.VMEM((n, GROUPS - 1, 2, 2, piece, wc), bf16),
            pltpu.VMEM((n, 2, 2, rows, wc), bf16),
            pltpu.VMEM((n, 2, 2, rows, wc), f32),
            pltpu.VMEM((n, 2, 2, rows, wc), f32),
            pltpu.VMEM((n, 2, 2, XS, 2 * rows, wc), bf16),
            pltpu.VMEM((n, 2, rows, wc), bf16),
            pltpu.VMEM((count, width), bf16),
            pltpu.VMEM((2 * count, width), bf16),
            pltpu.VMEM((n, 2 * count, wc), bf16),
            dma((n, 2)), dma((n, 2)), dma((n, 2)), dma((1,)),
            dma((n, GROUPS - 1)), dma((n, GROUPS - 1)),
            dma((n, GROUPS - 1)), dma((n, GROUPS - 1)),
            dma((n,)), dma((n,)), dma((1,)), dma((1,)),
            dma((n,)), dma((n,)),
            dma((n, 2)), dma((n, 2)), dma((n, 2)), dma((n, 2)),
            dma((n,)), dma((n,)), dma((n,)), dma((n, 2)),
        ],
        compiler_params=pltpu.CompilerParams(
            collective_id=0, has_side_effects=True, vmem_limit_bytes=60 * 2**20
        ),
        cost_estimate=pl.CostEstimate(
            flops=4 * count * width * cols, bytes_accessed=2**25, transcendentals=count * cols
        ),
    )(tokens, gain, params, moment, deltas)


def body(tokens, norm_gain, outer_params, momentum, deltas):
    sums, hidden = fused(
        tokens, norm_gain.reshape(1, -1), outer_params, momentum, deltas[0]
    )
    outer_grad = sums.astype(jnp.float32) * (1.0 / GROUPS)
    new_momentum = MU * momentum + outer_grad
    new_params = outer_params - RATE * (outer_grad + MU * new_momentum)
    return (new_params, new_momentum, hidden)


def solution(mesh):
    in_specs = (
        P(("rep", "fsdp"), None),
        P(),
        P(None, "fsdp", None),
        P(None, "fsdp", None),
        P("rep", None, "fsdp", None),
    )
    out_specs = (P(None, "fsdp", None), P(None, "fsdp", None), P(("rep", "fsdp"), None))
    return jax.shard_map(body, mesh=mesh, in_specs=in_specs, out_specs=out_specs, check_vma=False)
```

```python
import functools
import math

import jax
import jax.numpy as jnp
from jax import lax
from jax.experimental import pallas as pl
from jax.experimental.pallas import tpu as pltpu
from jax.sharding import PartitionSpec as P

EPS = 1e-05
MU = 0.9
RATE = 0.7
MESH = pl.DeviceIdType.MESH

CHUNKS = 8
GROUPS = 8
XS = 4
ZS = 4
PART_X = 96
PART_Y = 96
PART_Z = 64


def kernel(
    tok_ref, gain_ref, p_ref, m_ref, d_ref,
    sums_ref, hid_ref,
    dl, rs, sm, pb, mb, w, stg, tk, nt, ob,
    ld_d, ld_p, ld_m, ld_t,
    rs_s, rs_r, sm_s, sm_r, d2_s, d2_r, nt_s, nt_r,
    yo_s, yo_r, x_s, x_r, f_s, f_r, yi_s, yi_r, z_s, z_r, o_l, o_s, o_r, so_s,
):
    n = CHUNKS
    rows = dl.shape[3]
    wc = dl.shape[4]
    half = n * wc
    piece = rows // GROUPS
    tokens = tk.shape[0]
    width = tk.shape[1]

    rep = lax.axis_index("rep")
    fs = lax.axis_index("fsdp")
    core = lax.rem(fs, 2)
    other = 1 - core
    chip = fs // 2
    x = lax.rem(chip, XS)
    yh = chip // XS
    yl = lax.rem(rep, 2)
    z = rep // 2
    x_up = lax.rem(x + 1, XS)
    x_dn = lax.rem(x + XS - 1, XS)
    x_far = lax.rem(x + 2, XS)

    def fsdp_of(yh_, x_, core_):
        return (yh_ * XS + x_) * 2 + core_

    partner = (rep, fsdp_of(yh, x, other))
    across = (z * 2 + 1 - yl, fsdp_of(1 - yh, x, core))
    up = (rep, fsdp_of(yh, x_up, core))
    down = (rep, fsdp_of(yh, x_dn, core))
    beside = (z * 2 + 1 - yl, fs)
    layers = [(lax.rem(z + k, ZS) * 2 + yl, fs) for k in (1, 2, 3)]
    peers = [(lax.rem(rep + k, GROUPS), fs) for k in range(1, GROUPS)]

    def load(src, dst, sem, j, h):
        return pltpu.make_async_copy(
            src.at[:, :, pl.ds(pl.multiple_of(h * half + j * wc, wc), wc)],
            dst.at[j, h],
            sem.at[j, h],
        )

    def remote(src, dst, send, recv, device):
        return pltpu.make_async_remote_copy(
            src_ref=src, dst_ref=dst, send_sem=send, recv_sem=recv,
            device_id=device, device_id_type=MESH,
        )

    def rs_copy(j, k):
        rows_of = pl.multiple_of(peers[k][0] * piece, piece)
        return remote(
            dl.at[j, :, :, pl.ds(rows_of, piece), :], rs.at[j, k],
            rs_s.at[j, k], rs_r.at[j, k], peers[k],
        )

    def sm_copy(j, k):
        mine = pl.ds(pl.multiple_of(rep * piece, piece), piece)
        ref = sm.at[j, :, :, mine, :]
        return remote(ref, ref, sm_s.at[j, k], sm_r.at[j, k], peers[k])

    def d2_copy(j):
        at = pl.ds(pl.multiple_of(core * rows, rows), rows)
        return remote(
            stg.at[j], w.at[j, :, yh, x, at, :], d2_s.at[j], d2_r.at[j], partner
        )

    def part_x():
        return pl.ds(0, PART_X)

    def part_y(h):
        size = PART_Y // 2
        return pl.ds(pl.multiple_of(PART_X + h * size, 16), size)

    def part_z():
        size = PART_Z // ZS
        return pl.ds(pl.multiple_of(PART_X + PART_Y + z * size, 16), size)

    def yo_copy(j, i):
        ref = w.at[j, :, yh, x, (part_x(), part_y(1 - yl), part_z())[i], :]
        return remote(ref, ref, yo_s.at[j, i], yo_r.at[j, i], across)

    def x_copy(j, i, k):
        ref = w.at[j, :, :, x, (part_x(), part_y(yl), part_z())[i], :]
        return remote(ref, ref, x_s.at[j, i, k], x_r.at[j, i, k], (up, down)[k])

    def f_copy(j, i, k):
        ref = w.at[
            j, k, :, (x_dn, x_up)[k], (part_x(), part_y(yl), part_z())[i], :
        ]
        return remote(ref, ref, f_s.at[j, i, k], f_r.at[j, i, k], (up, down)[k])

    def block(j, b, at):
        if b == 0:
            return w.at[j, :, 1 - yh, x, at, :]
        return w.at[j, :, :, (x_up, x_dn, x_far)[b - 1], at, :]

    def yi_copy(j, b):
        ref = block(j, b, part_y(yl))
        return remote(ref, ref, yi_s.at[j, b], yi_r.at[j, b], beside)

    def z_copy(j, b, k):
        ref = block(j, b, part_z())
        return remote(ref, ref, z_s.at[j, b, k], z_r.at[j, b, k], layers[k])

    def share(j, b):
        yi_copy(j, b).start()
        for k in range(3):
            z_copy(j, b, k).start()

    def nt_copy():
        ref = nt.at[pl.ds(pl.multiple_of(core * tokens, tokens), tokens), :]
        return remote(ref, ref, nt_s.at[0], nt_r.at[0], partner)

    def column(j):
        return pl.ds(pl.multiple_of(core * half + j * wc, wc), wc)

    def own_out(j):
        at = pl.ds(pl.multiple_of(core * tokens, tokens), tokens)
        return pltpu.make_async_copy(
            ob.at[j, at, :], hid_ref.at[:, column(j)], o_l.at[j]
        )

    def far_out(j):
        at = pl.ds(pl.multiple_of(other * tokens, tokens), tokens)
        return remote(
            ob.at[j, at, :], hid_ref.at[:, column(j)], o_s.at[j], o_r.at[j], partner
        )

    def sums_out(j, h):
        return pltpu.make_async_copy(
            sm.at[j, h],
            sums_ref.at[:, :, pl.ds(pl.multiple_of(h * half + j * wc, wc), wc)],
            so_s.at[j, h],
        )

    def both(fn):
        for h in range(2):
            fn(h)

    @pl.loop(0, n)
    def _(j):
        both(lambda h: load(d_ref, dl, ld_d, j, h).start())

    pltpu.make_async_copy(tok_ref, tk, ld_t.at[0]).start()

    @pl.loop(0, n)
    def _(j):
        both(lambda h: load(p_ref, pb, ld_p, j, h).start())
        both(lambda h: load(m_ref, mb, ld_m, j, h).start())

    barrier = pltpu.get_barrier_semaphore()
    friends = peers + [partner, across, up, down]
    for friend in friends:
        pl.semaphore_signal(barrier, inc=1, device_id=friend, device_id_type=MESH)
    pl.semaphore_wait(barrier, len(friends))

    def scatter(j):
        both(lambda h: load(d_ref, dl, ld_d, j, h).wait())
        for k in range(GROUPS - 1):
            rs_copy(j, k).start()

    for j in range(2):
        scatter(j)

    pltpu.make_async_copy(tok_ref, tk, ld_t.at[0]).wait()
    step = 32

    @pl.loop(0, tokens // step)
    def _(i):
        at = pl.multiple_of(i * step, step)
        values = tk[pl.ds(at, step), :].astype(jnp.float32)
        mean = jnp.sum(values * values, axis=1, keepdims=True) * (1.0 / width)
        scaled = values * lax.rsqrt(mean + EPS) * gain_ref[...]
        base = pl.multiple_of(core * tokens + at, step)
        nt[pl.ds(base, step), :] = scaled.astype(jnp.bfloat16)

    def add_up(j):
        for k in range(GROUPS - 1):
            rs_copy(j, k).wait_recv()
        mine = pl.ds(pl.multiple_of(rep * piece, piece), piece)
        for h in range(2):
            for q in range(2):
                total = dl[j, h, q, mine, :].astype(jnp.float32)
                for k in range(GROUPS - 1):
                    total = total + rs[j, k, h, q].astype(jnp.float32)
                sm[j, h, q, mine, :] = total.astype(jnp.bfloat16)

    def update(j):
        for k in range(GROUPS - 1):
            sm_copy(j, k).wait_recv()
        both(lambda h: load(p_ref, pb, ld_p, j, h).wait())
        both(lambda h: load(m_ref, mb, ld_m, j, h).wait())
        at = pl.ds(pl.multiple_of(core * rows, rows), rows)

        def weights(h, q):
            grad = sm[j, h, q].astype(jnp.float32) * (1.0 / GROUPS)
            moment = MU * mb[j, h, q] + grad
            fresh = pb[j, h, q] - RATE * (grad + MU * moment)
            return fresh.astype(jnp.bfloat16)

        for q in range(2):
            stg[j, q] = weights(other, q)
        for q in range(2):
            w[j, q, yh, x, at, :] = weights(core, q)
        both(lambda h: sums_out(j, h).start())

    factor = 1.0 / math.sqrt(width)
    tile = 256

    def project(j):
        @pl.loop(0, 2 * tokens // tile)
        def _(i):
            at = pl.ds(pl.multiple_of(i * tile, tile), tile)
            left = nt[at, :]
            gate = jnp.dot(
                left, w[j, 0].reshape(width, wc), preferred_element_type=jnp.float32
            ) * factor
            raised = jnp.dot(
                left, w[j, 1].reshape(width, wc), preferred_element_type=jnp.float32
            ) * factor
            ob[j, at, :] = (gate / (1.0 + jnp.exp(-gate)) * raised).astype(jnp.bfloat16)

    nt_copy().start()

    @pl.loop(0, n + 6)
    def _(t):
        def stage(lag, fn):
            j = t - lag

            @pl.when(jnp.logical_and(j >= 0, j < n))
            def _():
                fn(j)

        def stage_x(j):
            for i in range(3):
                yo_copy(j, i).wait_recv()
            for i in range(3):
                for k in range(2):
                    x_copy(j, i, k).start()
            share(j, 0)

        def stage_y(j):
            d2_copy(j).wait_recv()
            for i in range(3):
                yo_copy(j, i).start()

        def stage_send_sums(j):
            for k in range(GROUPS - 1):
                sm_copy(j, k).start()

        def stage_forward(j):
            for k in range(2):
                for i in range(3):
                    x_copy(j, i, k).wait_recv()
            for i in range(3):
                for k in range(2):
                    f_copy(j, i, k).start()
            share(j, 1)
            share(j, 2)

        def stage_far(j):
            for k in range(2):
                for i in range(3):
                    f_copy(j, i, k).wait_recv()
            share(j, 3)

        def stage_project(j):
            for b in range(4):
                yi_copy(j, b).wait_recv()
                for k in range(3):
                    z_copy(j, b, k).wait_recv()

            @pl.when(j == 0)
            def _():
                nt_copy().wait_recv()

            project(j)
            own_out(j).start()
            far_out(j).start()

        stage(3, stage_x)
        stage(2, stage_y)
        stage(1, update)
        stage(0, add_up)
        stage(1, lambda j: d2_copy(j).start())
        stage(-2, scatter)
        stage(0, stage_send_sums)
        stage(4, stage_forward)
        stage(5, stage_far)
        stage(6, stage_project)

    nt_copy().wait_send()

    @pl.loop(0, n)
    def _(j):
        for k in range(GROUPS - 1):
            rs_copy(j, k).wait_send()
            sm_copy(j, k).wait_send()
        d2_copy(j).wait_send()
        for i in range(3):
            yo_copy(j, i).wait_send()
            for k in range(2):
                x_copy(j, i, k).wait_send()
                f_copy(j, i, k).wait_send()
        for b in range(4):
            yi_copy(j, b).wait_send()
            for k in range(3):
                z_copy(j, b, k).wait_send()
        both(lambda h: sums_out(j, h).wait())
        own_out(j).wait()
        far_out(j).wait_send()
        far_out(j).wait_recv()


def fused(tokens, gain, params, moment, deltas):
    count, width = tokens.shape
    _, rows, cols = params.shape
    n = CHUNKS
    wc = cols // (2 * n)
    piece = rows // GROUPS
    bf16, f32 = jnp.bfloat16, jnp.float32
    dma = pltpu.SemaphoreType.DMA
    any_spec = pl.BlockSpec(memory_space=pl.ANY)
    return pl.pallas_call(
        kernel,
        out_shape=(
            jax.ShapeDtypeStruct((2, rows, cols), bf16),
            jax.ShapeDtypeStruct((count, cols), bf16),
        ),
        in_specs=[any_spec, pl.BlockSpec(memory_space=pltpu.VMEM), any_spec, any_spec, any_spec],
        out_specs=(any_spec, any_spec),
        scratch_shapes=[
            pltpu.VMEM((n, 2, 2, rows, wc), bf16),
            pltpu.VMEM((n, GROUPS - 1, 2, 2, piece, wc), bf16),
            pltpu.VMEM((n, 2, 2, rows, wc), bf16),
            pltpu.VMEM((n, 2, 2, rows, wc), f32),
            pltpu.VMEM((n, 2, 2, rows, wc), f32),
            pltpu.VMEM((n, 2, 2, XS, 2 * rows, wc), bf16),
            pltpu.VMEM((n, 2, rows, wc), bf16),
            pltpu.VMEM((count, width), bf16),
            pltpu.VMEM((2 * count, width), bf16),
            pltpu.VMEM((n, 2 * count, wc), bf16),
            dma((n, 2)), dma((n, 2)), dma((n, 2)), dma((1,)),
            dma((n, GROUPS - 1)), dma((n, GROUPS - 1)),
            dma((n, GROUPS - 1)), dma((n, GROUPS - 1)),
            dma((n,)), dma((n,)), dma((1,)), dma((1,)),
            dma((n, 3)), dma((n, 3)),
            dma((n, 3, 2)), dma((n, 3, 2)), dma((n, 3, 2)), dma((n, 3, 2)),
            dma((n, 4)), dma((n, 4)), dma((n, 4, 3)), dma((n, 4, 3)),
            dma((n,)), dma((n,)), dma((n,)), dma((n, 2)),
        ],
        compiler_params=pltpu.CompilerParams(
            collective_id=0, has_side_effects=True, vmem_limit_bytes=60 * 2**20
        ),
        cost_estimate=pl.CostEstimate(
            flops=4 * count * width * cols, bytes_accessed=2**25, transcendentals=count * cols
        ),
    )(tokens, gain, params, moment, deltas)


def body(tokens, norm_gain, outer_params, momentum, deltas):
    sums, hidden = fused(
        tokens, norm_gain.reshape(1, -1), outer_params, momentum, deltas[0]
    )
    outer_grad = sums.astype(jnp.float32) * (1.0 / GROUPS)
    new_momentum = MU * momentum + outer_grad
    new_params = outer_params - RATE * (outer_grad + MU * new_momentum)
    return (new_params, new_momentum, hidden)


def solution(mesh):
    in_specs = (
        P(("rep", "fsdp"), None),
        P(),
        P(None, "fsdp", None),
        P(None, "fsdp", None),
        P("rep", None, "fsdp", None),
    )
    out_specs = (P(None, "fsdp", None), P(None, "fsdp", None), P(("rep", "fsdp"), None))
    return jax.shard_map(body, mesh=mesh, in_specs=in_specs, out_specs=out_specs, check_vma=False)
```

```python
import functools
import math

import jax
import jax.numpy as jnp
from jax import lax
from jax.experimental import pallas as pl
from jax.experimental.pallas import tpu as pltpu
from jax.sharding import PartitionSpec as P

EPS = 1e-05
MU = 0.9
RATE = 0.7
MESH = pl.DeviceIdType.MESH

CHUNKS = 8
GROUPS = 8
XS = 4
ZS = 4
PART_X = 64
PART_D = 64
PART_Y = 64
PART_Z = 64
NORM_STEPS = 4


def kernel(
    tok_ref, gain_ref, p_ref, m_ref, d_ref,
    sums_ref, hid_ref,
    dl, rs, sm, pb, mb, w, stg, tk, nt, ob,
    ld_d, ld_p, ld_m, ld_t,
    rs_s, rs_r, sm_s, sm_r, d2_s, d2_r, nt_s, nt_r,
    yo_s, yo_r, x_s, x_r, f_s, f_r, yi_s, yi_r, z_s, z_r,
    xd_s, xd_r, fd_s, fd_r, ac_s, ac_r, o_l, o_s, o_r, so_s,
):
    n = CHUNKS
    rows = dl.shape[3]
    wc = dl.shape[4]
    half = n * wc
    piece = rows // GROUPS
    tokens = tk.shape[0]
    width = tk.shape[1]

    rep = lax.axis_index("rep")
    fs = lax.axis_index("fsdp")
    core = lax.rem(fs, 2)
    other = 1 - core
    chip = fs // 2
    x = lax.rem(chip, XS)
    yh = chip // XS
    yl = lax.rem(rep, 2)
    z = rep // 2
    x_up = lax.rem(x + 1, XS)
    x_dn = lax.rem(x + XS - 1, XS)
    x_far = lax.rem(x + 2, XS)

    def fsdp_of(yh_, x_, core_):
        return (yh_ * XS + x_) * 2 + core_

    partner = (rep, fsdp_of(yh, x, other))
    across = (z * 2 + 1 - yl, fsdp_of(1 - yh, x, core))
    up = (rep, fsdp_of(yh, x_up, core))
    down = (rep, fsdp_of(yh, x_dn, core))
    beside = (z * 2 + 1 - yl, fs)
    layers = [(lax.rem(z + k, ZS) * 2 + yl, fs) for k in (1, 2, 3)]
    peers = [(lax.rem(rep + k, GROUPS), fs) for k in range(1, GROUPS)]

    def load(src, dst, sem, j, h):
        return pltpu.make_async_copy(
            src.at[:, :, pl.ds(pl.multiple_of(h * half + j * wc, wc), wc)],
            dst.at[j, h],
            sem.at[j, h],
        )

    def remote(src, dst, send, recv, device):
        return pltpu.make_async_remote_copy(
            src_ref=src, dst_ref=dst, send_sem=send, recv_sem=recv,
            device_id=device, device_id_type=MESH,
        )

    def rs_copy(j, k):
        rows_of = pl.multiple_of(peers[k][0] * piece, piece)
        return remote(
            dl.at[j, :, :, pl.ds(rows_of, piece), :], rs.at[j, k],
            rs_s.at[j, k], rs_r.at[j, k], peers[k],
        )

    def sm_copy(j, k):
        mine = pl.ds(pl.multiple_of(rep * piece, piece), piece)
        ref = sm.at[j, :, :, mine, :]
        return remote(ref, ref, sm_s.at[j, k], sm_r.at[j, k], peers[k])

    def d2_copy(j):
        at = pl.ds(pl.multiple_of(core * rows, rows), rows)
        return remote(
            stg.at[j], w.at[j, :, yh, x, at, :], d2_s.at[j], d2_r.at[j], partner
        )

    def part_x():
        return pl.ds(0, PART_X)

    def part_d():
        return pl.ds(PART_X, PART_D)

    def part_xd():
        return pl.ds(0, PART_X + PART_D)

    def part_y(h):
        size = PART_Y // 2
        return pl.ds(pl.multiple_of(PART_X + PART_D + h * size, 16), size)

    def part_z():
        size = PART_Z // ZS
        return pl.ds(pl.multiple_of(PART_X + PART_D + PART_Y + z * size, 16), size)

    def yo_copy(j, i):
        ref = w.at[j, :, yh, x, (part_xd(), part_y(1 - yl), part_z())[i], :]
        return remote(ref, ref, yo_s.at[j, i], yo_r.at[j, i], across)

    def x_copy(j, i, k):
        ref = w.at[j, :, :, x, (part_x(), part_y(yl), part_z())[i], :]
        return remote(ref, ref, x_s.at[j, i, k], x_r.at[j, i, k], (up, down)[k])

    def xd_copy(j, k):
        ref = w.at[j, :, yh, x, part_d(), :]
        return remote(ref, ref, xd_s.at[j, k], xd_r.at[j, k], (up, down)[k])

    def fd_copy(j, k):
        ref = w.at[j, k, yh, (x_dn, x_up)[k], part_d(), :]
        return remote(ref, ref, fd_s.at[j, k], fd_r.at[j, k], (up, down)[k])

    def ac_copy(j, b):
        ref = w.at[j, :, yh, (x_up, x_dn, x_far)[b - 1], part_d(), :]
        return remote(ref, ref, ac_s.at[j, b - 1], ac_r.at[j, b - 1], across)

    def f_copy(j, i, k):
        ref = w.at[
            j, k, :, (x_dn, x_up)[k], (part_x(), part_y(yl), part_z())[i], :
        ]
        return remote(ref, ref, f_s.at[j, i, k], f_r.at[j, i, k], (up, down)[k])

    def block(j, b, at):
        if b == 0:
            return w.at[j, :, 1 - yh, x, at, :]
        return w.at[j, :, :, (x_up, x_dn, x_far)[b - 1], at, :]

    def yi_copy(j, b):
        ref = block(j, b, part_y(yl))
        return remote(ref, ref, yi_s.at[j, b], yi_r.at[j, b], beside)

    def z_copy(j, b, k):
        ref = block(j, b, part_z())
        return remote(ref, ref, z_s.at[j, b, k], z_r.at[j, b, k], layers[k])

    def share(j, b):
        yi_copy(j, b).start()
        for k in range(3):
            z_copy(j, b, k).start()
        if b > 0:
            ac_copy(j, b).start()

    def nt_copy():
        ref = nt.at[pl.ds(pl.multiple_of(core * tokens, tokens), tokens), :]
        return remote(ref, ref, nt_s.at[0], nt_r.at[0], partner)

    def column(j):
        return pl.ds(pl.multiple_of(core * half + j * wc, wc), wc)

    def own_out(j):
        at = pl.ds(pl.multiple_of(core * tokens, tokens), tokens)
        return pltpu.make_async_copy(
            ob.at[j, at, :], hid_ref.at[:, column(j)], o_l.at[j]
        )

    def far_out(j):
        at = pl.ds(pl.multiple_of(other * tokens, tokens), tokens)
        return remote(
            ob.at[j, at, :], hid_ref.at[:, column(j)], o_s.at[j], o_r.at[j], partner
        )

    def sums_out(j, h):
        return pltpu.make_async_copy(
            sm.at[j, h],
            sums_ref.at[:, :, pl.ds(pl.multiple_of(h * half + j * wc, wc), wc)],
            so_s.at[j, h],
        )

    def both(fn):
        for h in range(2):
            fn(h)

    @pl.loop(0, n)
    def _(j):
        both(lambda h: load(d_ref, dl, ld_d, j, h).start())

    barrier = pltpu.get_barrier_semaphore()
    friends = peers + [partner, across, up, down]
    for friend in friends:
        pl.semaphore_signal(barrier, inc=1, device_id=friend, device_id_type=MESH)
    pl.semaphore_wait(barrier, len(friends))

    def scatter(j):
        both(lambda h: load(d_ref, dl, ld_d, j, h).wait())
        for k in range(GROUPS - 1):
            rs_copy(j, k).start()

    for j in range(2):
        scatter(j)

    pltpu.make_async_copy(tok_ref, tk, ld_t.at[0]).start()

    @pl.loop(0, n)
    def _(j):
        both(lambda h: load(p_ref, pb, ld_p, j, h).start())
        both(lambda h: load(m_ref, mb, ld_m, j, h).start())

    step = 16
    share_of = tokens // NORM_STEPS

    def norm(part):
        @pl.when(part == 0)
        def _():
            pltpu.make_async_copy(tok_ref, tk, ld_t.at[0]).wait()

        @pl.loop(0, share_of // step)
        def _(i):
            at = pl.multiple_of(part * share_of + i * step, step)
            values = tk[pl.ds(at, step), :].astype(jnp.float32)
            mean = jnp.sum(values * values, axis=1, keepdims=True) * (1.0 / width)
            scaled = values * lax.rsqrt(mean + EPS) * gain_ref[...]
            base = pl.multiple_of(core * tokens + at, step)
            nt[pl.ds(base, step), :] = scaled.astype(jnp.bfloat16)

    def add_up(j):
        for k in range(GROUPS - 1):
            rs_copy(j, k).wait_recv()
        mine = pl.ds(pl.multiple_of(rep * piece, piece), piece)
        for h in range(2):
            for q in range(2):
                total = dl[j, h, q, mine, :].astype(jnp.float32)
                for k in range(GROUPS - 1):
                    total = total + rs[j, k, h, q].astype(jnp.float32)
                sm[j, h, q, mine, :] = total.astype(jnp.bfloat16)

    def update(j):
        for k in range(GROUPS - 1):
            sm_copy(j, k).wait_recv()
        both(lambda h: load(p_ref, pb, ld_p, j, h).wait())
        both(lambda h: load(m_ref, mb, ld_m, j, h).wait())
        at = pl.ds(pl.multiple_of(core * rows, rows), rows)

        def weights(h, q):
            grad = sm[j, h, q].astype(jnp.float32) * (1.0 / GROUPS)
            moment = MU * mb[j, h, q] + grad
            fresh = pb[j, h, q] - RATE * (grad + MU * moment)
            return fresh.astype(jnp.bfloat16)

        for q in range(2):
            stg[j, q] = weights(other, q)
        for q in range(2):
            w[j, q, yh, x, at, :] = weights(core, q)
        both(lambda h: sums_out(j, h).start())

    factor = 1.0 / math.sqrt(width)
    tile = 256

    def project(j):
        @pl.loop(0, 2 * tokens // tile)
        def _(i):
            at = pl.ds(pl.multiple_of(i * tile, tile), tile)
            left = nt[at, :]
            gate = jnp.dot(
                left, w[j, 0].reshape(width, wc), preferred_element_type=jnp.float32
            ) * factor
            raised = jnp.dot(
                left, w[j, 1].reshape(width, wc), preferred_element_type=jnp.float32
            ) * factor
            ob[j, at, :] = (gate / (1.0 + jnp.exp(-gate)) * raised).astype(jnp.bfloat16)

    @pl.loop(0, n + 6)
    def _(t):
        def stage(lag, fn):
            j = t - lag

            @pl.when(jnp.logical_and(j >= 0, j < n))
            def _():
                fn(j)

        def stage_x(j):
            for i in range(3):
                yo_copy(j, i).wait_recv()
            for i in range(3):
                for k in range(2):
                    x_copy(j, i, k).start()
            share(j, 0)

        def stage_y(j):
            d2_copy(j).wait_recv()
            for i in range(3):
                yo_copy(j, i).start()
            for k in range(2):
                xd_copy(j, k).start()

        def stage_send_sums(j):
            for k in range(GROUPS - 1):
                sm_copy(j, k).start()

        def stage_forward(j):
            for k in range(2):
                xd_copy(j, k).wait_recv()
                for i in range(3):
                    x_copy(j, i, k).wait_recv()
            for k in range(2):
                fd_copy(j, k).start()
                for i in range(3):
                    f_copy(j, i, k).start()
            share(j, 1)
            share(j, 2)

        def stage_far(j):
            for k in range(2):
                fd_copy(j, k).wait_recv()
                for i in range(3):
                    f_copy(j, i, k).wait_recv()
            share(j, 3)

        def stage_project(j):
            for b in range(4):
                yi_copy(j, b).wait_recv()
                for k in range(3):
                    z_copy(j, b, k).wait_recv()
                if b > 0:
                    ac_copy(j, b).wait_recv()

            @pl.when(j == 0)
            def _():
                nt_copy().wait_recv()

            project(j)
            own_out(j).start()
            far_out(j).start()

        stage(3, stage_x)
        stage(2, stage_y)
        stage(1, update)
        stage(0, add_up)
        stage(1, lambda j: d2_copy(j).start())
        stage(-2, scatter)
        stage(0, stage_send_sums)
        @pl.when(t < NORM_STEPS)
        def _():
            norm(t)

        stage(4, stage_forward)

        @pl.when(t == NORM_STEPS)
        def _():
            nt_copy().start()

        stage(5, stage_far)
        stage(6, stage_project)

    nt_copy().wait_send()

    @pl.loop(0, n)
    def _(j):
        for k in range(GROUPS - 1):
            rs_copy(j, k).wait_send()
            sm_copy(j, k).wait_send()
        d2_copy(j).wait_send()
        for i in range(3):
            yo_copy(j, i).wait_send()
            for k in range(2):
                x_copy(j, i, k).wait_send()
                f_copy(j, i, k).wait_send()
        for b in range(4):
            yi_copy(j, b).wait_send()
            for k in range(3):
                z_copy(j, b, k).wait_send()
            if b > 0:
                ac_copy(j, b).wait_send()
        for k in range(2):
            xd_copy(j, k).wait_send()
            fd_copy(j, k).wait_send()
        both(lambda h: sums_out(j, h).wait())
        own_out(j).wait()
        far_out(j).wait_send()
        far_out(j).wait_recv()


def fused(tokens, gain, params, moment, deltas):
    count, width = tokens.shape
    _, rows, cols = params.shape
    n = CHUNKS
    wc = cols // (2 * n)
    piece = rows // GROUPS
    bf16, f32 = jnp.bfloat16, jnp.float32
    dma = pltpu.SemaphoreType.DMA
    any_spec = pl.BlockSpec(memory_space=pl.ANY)
    return pl.pallas_call(
        kernel,
        out_shape=(
            jax.ShapeDtypeStruct((2, rows, cols), bf16),
            jax.ShapeDtypeStruct((count, cols), bf16),
        ),
        in_specs=[any_spec, pl.BlockSpec(memory_space=pltpu.VMEM), any_spec, any_spec, any_spec],
        out_specs=(any_spec, any_spec),
        scratch_shapes=[
            pltpu.VMEM((n, 2, 2, rows, wc), bf16),
            pltpu.VMEM((n, GROUPS - 1, 2, 2, piece, wc), bf16),
            pltpu.VMEM((n, 2, 2, rows, wc), bf16),
            pltpu.VMEM((n, 2, 2, rows, wc), f32),
            pltpu.VMEM((n, 2, 2, rows, wc), f32),
            pltpu.VMEM((n, 2, 2, XS, 2 * rows, wc), bf16),
            pltpu.VMEM((n, 2, rows, wc), bf16),
            pltpu.VMEM((count, width), bf16),
            pltpu.VMEM((2 * count, width), bf16),
            pltpu.VMEM((n, 2 * count, wc), bf16),
            dma((n, 2)), dma((n, 2)), dma((n, 2)), dma((1,)),
            dma((n, GROUPS - 1)), dma((n, GROUPS - 1)),
            dma((n, GROUPS - 1)), dma((n, GROUPS - 1)),
            dma((n,)), dma((n,)), dma((1,)), dma((1,)),
            dma((n, 3)), dma((n, 3)),
            dma((n, 3, 2)), dma((n, 3, 2)), dma((n, 3, 2)), dma((n, 3, 2)),
            dma((n, 4)), dma((n, 4)), dma((n, 4, 3)), dma((n, 4, 3)),
            dma((n, 2)), dma((n, 2)), dma((n, 2)), dma((n, 2)), dma((n, 3)), dma((n, 3)),
            dma((n,)), dma((n,)), dma((n,)), dma((n, 2)),
        ],
        compiler_params=pltpu.CompilerParams(
            collective_id=0, has_side_effects=True, vmem_limit_bytes=60 * 2**20
        ),
        cost_estimate=pl.CostEstimate(
            flops=4 * count * width * cols, bytes_accessed=2**25, transcendentals=count * cols
        ),
    )(tokens, gain, params, moment, deltas)


def body(tokens, norm_gain, outer_params, momentum, deltas):
    sums, hidden = fused(
        tokens, norm_gain.reshape(1, -1), outer_params, momentum, deltas[0]
    )
    outer_grad = sums.astype(jnp.float32) * (1.0 / GROUPS)
    new_momentum = MU * momentum + outer_grad
    new_params = outer_params - RATE * (outer_grad + MU * new_momentum)
    return (new_params, new_momentum, hidden)


def solution(mesh):
    in_specs = (
        P(("rep", "fsdp"), None),
        P(),
        P(None, "fsdp", None),
        P(None, "fsdp", None),
        P("rep", None, "fsdp", None),
    )
    out_specs = (P(None, "fsdp", None), P(None, "fsdp", None), P(("rep", "fsdp"), None))
    return jax.shard_map(body, mesh=mesh, in_specs=in_specs, out_specs=out_specs, check_vma=False)
```

```python
import functools
import math

import jax
import jax.numpy as jnp
from jax import lax
from jax.experimental import pallas as pl
from jax.experimental.pallas import tpu as pltpu
from jax.sharding import PartitionSpec as P

EPS = 1e-05
MU = 0.9
RATE = 0.7
MESH = pl.DeviceIdType.MESH

CHUNKS = 16
WIDE = CHUNKS // 2
GROUPS = 8
XS = 4
ZS = 4
NORM_STEPS = 4
WAYS = "DYZX"
LAG_Y, LAG_X, LAG_F, LAG_FAR, LAG_P = 4, 6, 9, 12, 15


def kernel(
    tok_ref, gain_ref, p_ref, m_ref, d_ref,
    np_ref, nm_ref, hid_ref,
    dl, rs, sm, w, stg, tk, nt, ob,
    ld_d, ld_p, ld_m, ld_t,
    rs_s, rs_r, sm_s, sm_r, d2_s, d2_r, nt_s, nt_r,
    yo_s, yo_r, x_s, x_r, f_s, f_r, sh_s, sh_r, o_s, o_r,
):
    n = CHUNKS
    rows = dl.shape[3]
    wide = dl.shape[4]
    wc = w.shape[5]
    half = n * wc
    piece = rows // GROUPS
    tokens = tk.shape[0]
    width = tk.shape[1]

    rep = lax.axis_index("rep")
    fs = lax.axis_index("fsdp")
    core = lax.rem(fs, 2)
    other = 1 - core
    chip = fs // 2
    x = lax.rem(chip, XS)
    yh = chip // XS
    yl = lax.rem(rep, 2)
    z = rep // 2
    x_up = lax.rem(x + 1, XS)
    x_dn = lax.rem(x + XS - 1, XS)
    x_far = lax.rem(x + 2, XS)

    def fsdp_of(yh_, x_, core_):
        return (yh_ * XS + x_) * 2 + core_

    partner = (rep, fsdp_of(yh, x, other))
    across = (z * 2 + 1 - yl, fsdp_of(1 - yh, x, core))
    up = (rep, fsdp_of(yh, x_up, core))
    down = (rep, fsdp_of(yh, x_dn, core))
    beside = (z * 2 + 1 - yl, fs)
    layers = [(lax.rem(z + k, ZS) * 2 + yl, fs) for k in (1, 2, 3)]
    peers = [(lax.rem(rep + k, GROUPS), fs) for k in range(1, GROUPS)]

    def wide_columns(jj, h):
        return pl.ds(pl.multiple_of(h * half + jj * wide, wide), wide)

    def load(src, dst, sem, jj, h):
        return pltpu.make_async_copy(
            src.at[:, :, wide_columns(jj, h)], dst.at[jj, h], sem.at[jj, h]
        )

    def load_state(src, dst, sem, jj, h):
        at = wide_columns(jj, h)
        return pltpu.make_async_copy(
            src.at[:, :, at], dst.at[:, :, at], sem.at[jj, h]
        )

    def remote(src, dst, send, recv, device):
        return pltpu.make_async_remote_copy(
            src_ref=src, dst_ref=dst, send_sem=send, recv_sem=recv,
            device_id=device, device_id_type=MESH,
        )

    def rs_copy(jj, k):
        rows_of = pl.multiple_of(peers[k][0] * piece, piece)
        return remote(
            dl.at[jj, :, :, pl.ds(rows_of, piece), :], rs.at[jj, k],
            rs_s.at[jj, k], rs_r.at[jj, k], peers[k],
        )

    def sm_copy(jj, k):
        mine = pl.ds(pl.multiple_of(rep * piece, piece), piece)
        ref = sm.at[jj, :, :, mine, :]
        return remote(ref, ref, sm_s.at[jj, k], sm_r.at[jj, k], peers[k])

    def d2_copy(jj):
        at = pl.ds(pl.multiple_of(core * rows, rows), rows)
        pair = pl.ds(2 * jj, 2)
        return remote(
            stg.at[pair], w.at[pair, :, yh, x, at, :], d2_s.at[jj], d2_r.at[jj], partner
        )

    def rows_all():
        return pl.ds(0, 2 * rows)

    def rows_half(h):
        return pl.ds(pl.multiple_of(h * rows, rows), rows)

    def rows_quarter():
        size = 2 * rows // ZS
        return pl.ds(pl.multiple_of(z * size, size), size)

    def part(way):
        if way == "Y":
            return rows_half(yl)
        if way == "Z":
            return rows_quarter()
        return rows_all()

    def yo_copy(way, j):
        at = rows_half(1 - yl) if way == "Y" else part(way)
        ref = w.at[j, :, yh, x, at, :]
        return remote(ref, ref, yo_s.at[j], yo_r.at[j], across)

    def x_copy(way, j, k):
        if way == "D":
            ref = w.at[j, :, yh, x]
        else:
            ref = w.at[j, :, :, x, part(way), :]
        return remote(ref, ref, x_s.at[j, k], x_r.at[j, k], (up, down)[k])

    def f_copy(way, j, k):
        from_x = (x_dn, x_up)[k]
        if way == "D":
            ref = w.at[j, k, yh, from_x]
        else:
            ref = w.at[j, k, :, from_x, part(way), :]
        return remote(ref, ref, f_s.at[j, k], f_r.at[j, k], (up, down)[k])

    def last_legs(way, j, b):
        from_x = (x, x_up, x_dn, x_far)[b]
        if way == "X":
            return []
        if way == "D":
            if b == 0:
                return [yo_copy(way, j)]
            ref = w.at[j, :, yh, from_x]
            return [remote(ref, ref, sh_s.at[j, b, 0], sh_r.at[j, b, 0], across)]
        if b == 0:
            ref = w.at[j, :, 1 - yh, x, part(way), :]
        else:
            ref = w.at[j, :, :, from_x, part(way), :]
        targets = [beside] if way == "Y" else layers
        return [
            remote(ref, ref, sh_s.at[j, b, k], sh_r.at[j, b, k], target)
            for k, target in enumerate(targets)
        ]

    def share(way, j, b):
        for copy in last_legs(way, j, b):
            copy.start()

    def nt_copy():
        ref = nt.at[pl.ds(pl.multiple_of(core * tokens, tokens), tokens), :]
        return remote(ref, ref, nt_s.at[0], nt_r.at[0], partner)

    def column(j):
        return pl.ds(pl.multiple_of(core * half + j * wc, wc), wc)

    def far_out(j):
        return remote(
            ob.at[j], hid_ref.at[:, column(j)], o_s.at[j], o_r.at[j], partner
        )

    def both(fn):
        for h in range(2):
            fn(h)

    @pl.loop(0, WIDE)
    def _(jj):
        both(lambda h: load(d_ref, dl, ld_d, jj, h).start())

    barrier = pltpu.get_barrier_semaphore()
    friends = peers + [partner, across, up, down]
    for friend in friends:
        pl.semaphore_signal(barrier, inc=1, device_id=friend, device_id_type=MESH)
    pl.semaphore_wait(barrier, len(friends))

    def scatter(jj):
        both(lambda h: load(d_ref, dl, ld_d, jj, h).wait())
        for k in range(GROUPS - 1):
            rs_copy(jj, k).start()

    for jj in range(2):
        scatter(jj)

    pltpu.make_async_copy(tok_ref, tk, ld_t.at[0]).start()

    @pl.loop(0, WIDE)
    def _(jj):
        both(lambda h: load_state(p_ref, np_ref, ld_p, jj, h).start())
        both(lambda h: load_state(m_ref, nm_ref, ld_m, jj, h).start())

    step = 16
    share_of = tokens // NORM_STEPS

    def norm(index):
        if index == 0:
            pltpu.make_async_copy(tok_ref, tk, ld_t.at[0]).wait()

        @pl.loop(0, share_of // step)
        def _(i):
            at = pl.multiple_of(index * share_of + i * step, step)
            values = tk[pl.ds(at, step), :].astype(jnp.float32)
            mean = jnp.sum(values * values, axis=1, keepdims=True) * (1.0 / width)
            scaled = values * lax.rsqrt(mean + EPS) * gain_ref[...]
            base = pl.multiple_of(core * tokens + at, step)
            nt[pl.ds(base, step), :] = scaled.astype(jnp.bfloat16)

    def add_up(jj):
        for k in range(GROUPS - 1):
            rs_copy(jj, k).wait_recv()
        mine = pl.ds(pl.multiple_of(rep * piece, piece), piece)
        for h in range(2):
            for q in range(2):
                total = dl[jj, h, q, mine, :].astype(jnp.float32)
                for k in range(GROUPS - 1):
                    total = total + rs[jj, k, h, q].astype(jnp.float32)
                sm[jj, h, q, mine, :] = total.astype(jnp.bfloat16)

    def send_sums(jj):
        for k in range(GROUPS - 1):
            sm_copy(jj, k).start()

    def update(jj):
        for k in range(GROUPS - 1):
            sm_copy(jj, k).wait_recv()
        both(lambda h: load_state(p_ref, np_ref, ld_p, jj, h).wait())
        both(lambda h: load_state(m_ref, nm_ref, ld_m, jj, h).wait())
        at = pl.ds(pl.multiple_of(core * rows, rows), rows)

        def weights(h, q):
            grad = sm[jj, h, q].astype(jnp.float32) * (1.0 / GROUPS)
            cols = wide_columns(jj, h)
            moment = MU * nm_ref[q, :, cols] + grad
            fresh = np_ref[q, :, cols] - RATE * (grad + MU * moment)
            nm_ref[q, :, cols] = moment
            np_ref[q, :, cols] = fresh
            return fresh.astype(jnp.bfloat16)

        for q in range(2):
            fresh = weights(other, q)
            for i in range(2):
                stg[2 * jj + i, q] = fresh[:, i * wc:(i + 1) * wc]
        for q in range(2):
            fresh = weights(core, q)
            for i in range(2):
                w[2 * jj + i, q, yh, x, at, :] = fresh[:, i * wc:(i + 1) * wc]

    def hand_over(jj):
        d2_copy(jj).start()

    factor = 1.0 / math.sqrt(width)
    tile = 256

    def project(j):
        def piece_of(base, i):
            left = nt[pl.ds(pl.multiple_of(base * tokens + i * tile, tile), tile), :]
            right = jnp.concatenate(
                [w[j, 0].reshape(width, wc), w[j, 1].reshape(width, wc)], axis=1
            )
            sums = jnp.dot(left, right, preferred_element_type=jnp.float32) * factor
            gate, raised = sums[:, :wc], sums[:, wc:]
            return (gate / (1.0 + jnp.exp(-gate)) * raised).astype(jnp.bfloat16)

        @pl.loop(0, tokens // tile)
        def _(i):
            at = pl.ds(pl.multiple_of(i * tile, tile), tile)
            ob[j, at, :] = piece_of(other, i)

        far_out(j).start()

        @pl.loop(0, tokens // tile)
        def _(i):
            at = pl.ds(pl.multiple_of(i * tile, tile), tile)
            hid_ref[at, column(j)] = piece_of(core, i)

    def stage_y(way, j, first):
        if first:
            d2_copy(j // 2).wait_recv()
        yo_copy(way, j).start()
        if way == "D":
            for k in range(2):
                x_copy(way, j, k).start()

    def stage_x(way, j):
        if way == "D":
            return
        yo_copy(way, j).wait_recv()
        for k in range(2):
            x_copy(way, j, k).start()
        share(way, j, 0)

    def stage_forward(way, j):
        for k in range(2):
            x_copy(way, j, k).wait_recv()
        for k in range(2):
            f_copy(way, j, k).start()
        share(way, j, 1)
        share(way, j, 2)

    def stage_far(way, j):
        for k in range(2):
            f_copy(way, j, k).wait_recv()
        share(way, j, 3)

    def stage_project(way, j):
        for b in range(4):
            for copy in last_legs(way, j, b):
                copy.wait_recv()
        project(j)

    cycle = len(WAYS)
    turns = -(-(n + LAG_P) // cycle)

    @pl.loop(0, turns)
    def _(turn):
        for slot in range(cycle):
            t = turn * cycle + slot

            def stage(lag, fn):
                j = t - lag
                way = WAYS[(slot - lag) % cycle]

                @pl.when(jnp.logical_and(j >= 0, j < n))
                def _():
                    fn(way, j)

            def wide_stage(ahead, fn):
                jj = t // 2 + ahead

                @pl.when(jnp.logical_and(jj >= 0, jj < WIDE))
                def _():
                    fn(jj)

            stage(LAG_X, stage_x)
            stage(LAG_Y, lambda way, j: stage_y(way, j, (slot - LAG_Y) % 2 == 0))
            if slot % 2 == 1:
                wide_stage(-1, update)
            else:
                wide_stage(0, add_up)
                wide_stage(0, send_sums)
                wide_stage(2, scatter)
            for index in range(NORM_STEPS):
                if index % cycle == slot:

                    @pl.when(t == index)
                    def _():
                        norm(index)

            if NORM_STEPS % cycle == slot:

                @pl.when(t == NORM_STEPS)
                def _():
                    nt_copy().start()

            if slot % 2 == 1:
                wide_stage(-1, hand_over)
            stage(LAG_F, stage_forward)
            stage(LAG_FAR, stage_far)
            if LAG_P % cycle == slot:

                @pl.when(t == LAG_P)
                def _():
                    nt_copy().wait_recv()

            stage(LAG_P, stage_project)

    nt_copy().wait_send()

    @pl.loop(0, WIDE)
    def _(jj):
        for k in range(GROUPS - 1):
            rs_copy(jj, k).wait_send()
            sm_copy(jj, k).wait_send()
        d2_copy(jj).wait_send()

    @pl.loop(0, n // cycle)
    def _(turn):
        for slot, way in enumerate(WAYS):
            j = turn * cycle + slot
            if way != "D":
                yo_copy(way, j).wait_send()
            for k in range(2):
                x_copy(way, j, k).wait_send()
                f_copy(way, j, k).wait_send()
            for b in range(4):
                for copy in last_legs(way, j, b):
                    copy.wait_send()
            far_out(j).wait_send()
            far_out(j).wait_recv()


def fused(tokens, gain, params, moment, deltas):
    count, width = tokens.shape
    _, rows, cols = params.shape
    n = CHUNKS
    wc = cols // (2 * n)
    wide = 2 * wc
    piece = rows // GROUPS
    bf16, f32 = jnp.bfloat16, jnp.float32
    dma = pltpu.SemaphoreType.DMA
    any_spec = pl.BlockSpec(memory_space=pl.ANY)
    return pl.pallas_call(
        kernel,
        out_shape=(
            pltpu.VMEM((2, rows, cols), f32),
            pltpu.VMEM((2, rows, cols), f32),
            pltpu.VMEM((count, cols), bf16),
        ),
        in_specs=[any_spec, pl.BlockSpec(memory_space=pltpu.VMEM), any_spec, any_spec, any_spec],
        out_specs=(pl.BlockSpec(memory_space=pltpu.VMEM),) * 3,
        scratch_shapes=[
            pltpu.VMEM((WIDE, 2, 2, rows, wide), bf16),
            pltpu.VMEM((WIDE, GROUPS - 1, 2, 2, piece, wide), bf16),
            pltpu.VMEM((WIDE, 2, 2, rows, wide), bf16),
            pltpu.VMEM((n, 2, 2, XS, 2 * rows, wc), bf16),
            pltpu.VMEM((n, 2, rows, wc), bf16),
            pltpu.VMEM((count, width), bf16),
            pltpu.VMEM((2 * count, width), bf16),
            pltpu.VMEM((n, count, wc), bf16),
            dma((WIDE, 2)), dma((WIDE, 2)), dma((WIDE, 2)), dma((1,)),
            dma((WIDE, GROUPS - 1)), dma((WIDE, GROUPS - 1)),
            dma((WIDE, GROUPS - 1)), dma((WIDE, GROUPS - 1)),
            dma((WIDE,)), dma((WIDE,)), dma((1,)), dma((1,)),
            dma((n,)), dma((n,)),
            dma((n, 2)), dma((n, 2)), dma((n, 2)), dma((n, 2)),
            dma((n, 4, 3)), dma((n, 4, 3)),
            dma((n,)), dma((n,)),
        ],
        compiler_params=pltpu.CompilerParams(
            collective_id=0, has_side_effects=True, vmem_limit_bytes=50 * 2**20
        ),
        cost_estimate=pl.CostEstimate(
            flops=4 * count * width * cols, bytes_accessed=2**25, transcendentals=count * cols
        ),
    )(tokens, gain, params, moment, deltas)


def body(tokens, norm_gain, outer_params, momentum, deltas):
    return fused(tokens, norm_gain.reshape(1, -1), outer_params, momentum, deltas[0])


def solution(mesh):
    in_specs = (
        P(("rep", "fsdp"), None),
        P(),
        P(None, "fsdp", None),
        P(None, "fsdp", None),
        P("rep", None, "fsdp", None),
    )
    out_specs = (P(None, "fsdp", None), P(None, "fsdp", None), P(("rep", "fsdp"), None))
    return jax.shard_map(body, mesh=mesh, in_specs=in_specs, out_specs=out_specs, check_vma=False)
```

```python
import functools
import math

import jax
import jax.numpy as jnp
from jax import lax
from jax.experimental import pallas as pl
from jax.experimental.pallas import tpu as pltpu
from jax.sharding import PartitionSpec as P

EPS = 1e-05
MU = 0.9
RATE = 0.7
MESH = pl.DeviceIdType.MESH

CHUNKS = 16
WIDE = CHUNKS // 2
GROUPS = 8
XS = 4
ZS = 4
NORM_STEPS = 4
WAYS = "DYZX"
LAG_Y, LAG_X, LAG_F, LAG_FAR, LAG_P = 4, 6, 8, 10, 12


def kernel(
    tok_ref, gain_ref, p_ref, m_ref, d_ref,
    np_ref, nm_ref, hid_ref,
    dl, rs, sm, w, stg, tk, nt, ob,
    ld_d, ld_p, ld_m, ld_t,
    rs_s, rs_r, sm_s, sm_r, d2_s, d2_r, nt_s, nt_r,
    yo_s, yo_r, x_s, x_r, f_s, f_r, sh_s, sh_r, o_s, o_r,
):
    n = CHUNKS
    rows = dl.shape[3]
    wide = dl.shape[4]
    wc = w.shape[5]
    half = n * wc
    piece = rows // GROUPS
    tokens = tk.shape[0]
    width = tk.shape[1]

    rep = lax.axis_index("rep")
    fs = lax.axis_index("fsdp")
    core = lax.rem(fs, 2)
    other = 1 - core
    chip = fs // 2
    x = lax.rem(chip, XS)
    yh = chip // XS
    yl = lax.rem(rep, 2)
    z = rep // 2
    x_up = lax.rem(x + 1, XS)
    x_dn = lax.rem(x + XS - 1, XS)
    x_far = lax.rem(x + 2, XS)

    def fsdp_of(yh_, x_, core_):
        return (yh_ * XS + x_) * 2 + core_

    partner = (rep, fsdp_of(yh, x, other))
    across = (z * 2 + 1 - yl, fsdp_of(1 - yh, x, core))
    up = (rep, fsdp_of(yh, x_up, core))
    down = (rep, fsdp_of(yh, x_dn, core))
    beside = (z * 2 + 1 - yl, fs)
    layers = [(lax.rem(z + k, ZS) * 2 + yl, fs) for k in (1, 2, 3)]
    peers = [(lax.rem(rep + k, GROUPS), fs) for k in range(1, GROUPS)]

    def wide_columns(jj, h):
        return pl.ds(pl.multiple_of(h * half + jj * wide, wide), wide)

    def load(src, dst, sem, jj, h):
        return pltpu.make_async_copy(
            src.at[:, :, wide_columns(jj, h)], dst.at[jj, h], sem.at[jj, h]
        )

    def load_state(src, dst, sem, jj, h):
        at = wide_columns(jj, h)
        return pltpu.make_async_copy(
            src.at[:, :, at], dst.at[:, :, at], sem.at[jj, h]
        )

    def remote(src, dst, send, recv, device):
        return pltpu.make_async_remote_copy(
            src_ref=src, dst_ref=dst, send_sem=send, recv_sem=recv,
            device_id=device, device_id_type=MESH,
        )

    def rs_copy(jj, k):
        rows_of = pl.multiple_of(peers[k][0] * piece, piece)
        return remote(
            dl.at[jj, :, :, pl.ds(rows_of, piece), :], rs.at[jj, k],
            rs_s.at[jj], rs_r.at[jj], peers[k],
        )

    def sm_copy(jj, k):
        mine = pl.ds(pl.multiple_of(rep * piece, piece), piece)
        ref = sm.at[jj, :, :, mine, :]
        return remote(ref, ref, sm_s.at[jj], sm_r.at[jj], peers[k])

    def d2_copy(jj):
        at = pl.ds(pl.multiple_of(core * rows, rows), rows)
        pair = pl.ds(2 * jj, 2)
        return remote(
            stg.at[pair], w.at[pair, :, yh, x, at, :], d2_s.at[jj], d2_r.at[jj], partner
        )

    def rows_all():
        return pl.ds(0, 2 * rows)

    def rows_half(h):
        return pl.ds(pl.multiple_of(h * rows, rows), rows)

    def rows_quarter():
        size = 2 * rows // ZS
        return pl.ds(pl.multiple_of(z * size, size), size)

    def part(way):
        if way == "Y":
            return rows_half(yl)
        if way == "Z":
            return rows_quarter()
        return rows_all()

    def yo_copy(way, j):
        at = rows_half(1 - yl) if way == "Y" else part(way)
        ref = w.at[j, :, yh, x, at, :]
        return remote(ref, ref, yo_s.at[j], yo_r.at[j], across)

    def x_copy(way, j, k):
        if way == "D":
            ref = w.at[j, :, yh, x]
        else:
            ref = w.at[j, :, :, x, part(way), :]
        return remote(ref, ref, x_s.at[j], x_r.at[j], (up, down)[k])

    def f_copy(way, j, k):
        from_x = (x_dn, x_up)[k]
        if way == "D":
            ref = w.at[j, k, yh, from_x]
        else:
            ref = w.at[j, k, :, from_x, part(way), :]
        return remote(ref, ref, f_s.at[j], f_r.at[j], (up, down)[k])

    def last_legs(way, j, b):
        from_x = (x, x_up, x_dn, x_far)[b]
        if way == "X":
            return []
        if way == "D":
            if b == 0:
                return [yo_copy(way, j)]
            ref = w.at[j, :, yh, from_x]
            return [remote(ref, ref, sh_s.at[j, b], sh_r.at[j, b], across)]
        if b == 0:
            ref = w.at[j, :, 1 - yh, x, part(way), :]
        else:
            ref = w.at[j, :, :, from_x, part(way), :]
        targets = [beside] if way == "Y" else layers
        return [
            remote(ref, ref, sh_s.at[j, b], sh_r.at[j, b], target)
            for k, target in enumerate(targets)
        ]

    def rs_all(jj):
        return remote(rs.at[jj], rs.at[jj], rs_s.at[jj], rs_r.at[jj], partner)

    def sm_all(jj):
        return remote(rs.at[jj], rs.at[jj], sm_s.at[jj], sm_r.at[jj], partner)

    def x_all(way, j):
        if way == "D":
            ref = w.at[j, :, 0, pl.ds(0, 2)]
        else:
            ref = w.at[j, :, :, pl.ds(0, 2), part(way), :]
        return remote(ref, ref, x_s.at[j], x_r.at[j], partner)

    def f_all(way, j):
        if way == "D":
            ref = w.at[j, 0, 0, pl.ds(0, 2)]
        else:
            ref = w.at[j, 0, :, pl.ds(0, 2), part(way), :]
        return remote(ref, ref, f_s.at[j], f_r.at[j], partner)

    def last_all(way, j, b):
        if way != "Z":
            return last_legs(way, j, b)
        if b == 0:
            ref = w.at[j, :, 0, pl.ds(0, 3), part(way), :]
        else:
            ref = w.at[j, :, :, pl.ds(0, 3), part(way), :]
        return [remote(ref, ref, sh_s.at[j, b], sh_r.at[j, b], partner)]

    def share(way, j, b):
        for copy in last_legs(way, j, b):
            copy.start()

    def nt_copy():
        ref = nt.at[pl.ds(pl.multiple_of(core * tokens, tokens), tokens), :]
        return remote(ref, ref, nt_s.at[0], nt_r.at[0], partner)

    def column(j):
        return pl.ds(pl.multiple_of(core * half + j * wc, wc), wc)

    def far_out(j):
        return remote(
            ob.at[j], hid_ref.at[:, column(j)], o_s.at[j], o_r.at[j], partner
        )

    def both(fn):
        for h in range(2):
            fn(h)

    @pl.loop(0, WIDE)
    def _(jj):
        both(lambda h: load(d_ref, dl, ld_d, jj, h).start())

    barrier = pltpu.get_barrier_semaphore()
    friends = peers + [partner, across, up, down]
    for friend in friends:
        pl.semaphore_signal(barrier, inc=1, device_id=friend, device_id_type=MESH)
    pl.semaphore_wait(barrier, len(friends))

    def scatter(jj):
        both(lambda h: load(d_ref, dl, ld_d, jj, h).wait())
        for k in range(GROUPS - 1):
            rs_copy(jj, k).start()

    for jj in range(2):
        scatter(jj)

    pltpu.make_async_copy(tok_ref, tk, ld_t.at[0]).start()

    @pl.loop(0, WIDE)
    def _(jj):
        both(lambda h: load_state(p_ref, np_ref, ld_p, jj, h).start())
        both(lambda h: load_state(m_ref, nm_ref, ld_m, jj, h).start())

    step = 16
    share_of = tokens // NORM_STEPS

    def norm(index):
        if index == 0:
            pltpu.make_async_copy(tok_ref, tk, ld_t.at[0]).wait()

        @pl.loop(0, share_of // step)
        def _(i):
            at = pl.multiple_of(index * share_of + i * step, step)
            values = tk[pl.ds(at, step), :].astype(jnp.float32)
            mean = jnp.sum(values * values, axis=1, keepdims=True) * (1.0 / width)
            scaled = values * lax.rsqrt(mean + EPS) * gain_ref[...]
            base = pl.multiple_of(core * tokens + at, step)
            nt[pl.ds(base, step), :] = scaled.astype(jnp.bfloat16)

    def add_up(jj):
        rs_all(jj).wait_recv()
        mine = pl.ds(pl.multiple_of(rep * piece, piece), piece)
        for h in range(2):
            for q in range(2):
                total = dl[jj, h, q, mine, :].astype(jnp.float32)
                for k in range(GROUPS - 1):
                    total = total + rs[jj, k, h, q].astype(jnp.float32)
                sm[jj, h, q, mine, :] = total.astype(jnp.bfloat16)

    def send_sums(jj):
        for k in range(GROUPS - 1):
            sm_copy(jj, k).start()

    def update(jj):
        sm_all(jj).wait_recv()
        both(lambda h: load_state(p_ref, np_ref, ld_p, jj, h).wait())
        both(lambda h: load_state(m_ref, nm_ref, ld_m, jj, h).wait())
        at = pl.ds(pl.multiple_of(core * rows, rows), rows)

        def weights(h, q):
            grad = sm[jj, h, q].astype(jnp.float32) * (1.0 / GROUPS)
            cols = wide_columns(jj, h)
            moment = MU * nm_ref[q, :, cols] + grad
            fresh = np_ref[q, :, cols] - RATE * (grad + MU * moment)
            nm_ref[q, :, cols] = moment
            np_ref[q, :, cols] = fresh
            return fresh.astype(jnp.bfloat16)

        for q in range(2):
            fresh = weights(other, q)
            for i in range(2):
                stg[2 * jj + i, q] = fresh[:, i * wc:(i + 1) * wc]
        for q in range(2):
            fresh = weights(core, q)
            for i in range(2):
                w[2 * jj + i, q, yh, x, at, :] = fresh[:, i * wc:(i + 1) * wc]

    def hand_over(jj):
        d2_copy(jj).start()

    factor = 1.0 / math.sqrt(width)
    tile = 256

    def project(j):
        def piece_of(base, i):
            left = nt[pl.ds(pl.multiple_of(base * tokens + i * tile, tile), tile), :]
            right = jnp.concatenate(
                [w[j, 0].reshape(width, wc), w[j, 1].reshape(width, wc)], axis=1
            )
            sums = jnp.dot(left, right, preferred_element_type=jnp.float32) * factor
            gate, raised = sums[:, :wc], sums[:, wc:]
            return (gate / (1.0 + jnp.exp(-gate)) * raised).astype(jnp.bfloat16)

        @pl.loop(0, tokens // tile)
        def _(i):
            at = pl.ds(pl.multiple_of(i * tile, tile), tile)
            ob[j, at, :] = piece_of(other, i)

        far_out(j).start()

        @pl.loop(0, tokens // tile)
        def _(i):
            at = pl.ds(pl.multiple_of(i * tile, tile), tile)
            hid_ref[at, column(j)] = piece_of(core, i)

    def stage_y(way, j, first):
        if first:
            d2_copy(j // 2).wait_recv()
        yo_copy(way, j).start()
        if way == "D":
            for k in range(2):
                x_copy(way, j, k).start()

    def stage_x(way, j):
        if way == "D":
            return
        yo_copy(way, j).wait_recv()
        for k in range(2):
            x_copy(way, j, k).start()
        share(way, j, 0)

    def stage_forward(way, j):
        x_all(way, j).wait_recv()
        for k in range(2):
            f_copy(way, j, k).start()
        share(way, j, 1)
        share(way, j, 2)

    def stage_far(way, j):
        f_all(way, j).wait_recv()
        share(way, j, 3)

    def stage_project(way, j):
        for b in range(4):
            for copy in last_all(way, j, b):
                copy.wait_recv()
        project(j)

    cycle = len(WAYS)
    turns = -(-(n + LAG_P) // cycle)

    @pl.loop(0, turns)
    def _(turn):
        for slot in range(cycle):
            t = turn * cycle + slot

            def stage(lag, fn):
                j = t - lag
                way = WAYS[(slot - lag) % cycle]

                @pl.when(jnp.logical_and(j >= 0, j < n))
                def _():
                    fn(way, j)

            def wide_stage(ahead, fn):
                jj = t // 2 + ahead

                @pl.when(jnp.logical_and(jj >= 0, jj < WIDE))
                def _():
                    fn(jj)

            stage(LAG_X, stage_x)
            stage(LAG_Y, lambda way, j: stage_y(way, j, (slot - LAG_Y) % 2 == 0))
            if slot % 2 == 1:
                wide_stage(-1, update)
            else:
                wide_stage(0, add_up)
                wide_stage(0, send_sums)
                wide_stage(2, scatter)
            for index in range(NORM_STEPS):
                if index % cycle == slot:

                    @pl.when(t == index)
                    def _():
                        norm(index)

            if NORM_STEPS % cycle == slot:

                @pl.when(t == NORM_STEPS)
                def _():
                    nt_copy().start()

            if slot % 2 == 1:
                wide_stage(-1, hand_over)
            stage(LAG_F, stage_forward)
            stage(LAG_FAR, stage_far)
            if LAG_P % cycle == slot:

                @pl.when(t == LAG_P)
                def _():
                    nt_copy().wait_recv()

            stage(LAG_P, stage_project)

    nt_copy().wait_send()

    @pl.loop(0, WIDE)
    def _(jj):
        rs_all(jj).wait_send()
        sm_all(jj).wait_send()
        d2_copy(jj).wait_send()

    @pl.loop(0, n // cycle)
    def _(turn):
        for slot, way in enumerate(WAYS):
            j = turn * cycle + slot
            if way != "D":
                yo_copy(way, j).wait_send()
            x_all(way, j).wait_send()
            f_all(way, j).wait_send()
            for b in range(4):
                for copy in last_all(way, j, b):
                    copy.wait_send()
            far_out(j).wait_send()
            far_out(j).wait_recv()


def fused(tokens, gain, params, moment, deltas):
    count, width = tokens.shape
    _, rows, cols = params.shape
    n = CHUNKS
    wc = cols // (2 * n)
    wide = 2 * wc
    piece = rows // GROUPS
    bf16, f32 = jnp.bfloat16, jnp.float32
    dma = pltpu.SemaphoreType.DMA
    any_spec = pl.BlockSpec(memory_space=pl.ANY)
    return pl.pallas_call(
        kernel,
        out_shape=(
            pltpu.VMEM((2, rows, cols), f32),
            pltpu.VMEM((2, rows, cols), f32),
            pltpu.VMEM((count, cols), bf16),
        ),
        in_specs=[any_spec, pl.BlockSpec(memory_space=pltpu.VMEM), any_spec, any_spec, any_spec],
        out_specs=(pl.BlockSpec(memory_space=pltpu.VMEM),) * 3,
        scratch_shapes=[
            pltpu.VMEM((WIDE, 2, 2, rows, wide), bf16),
            pltpu.VMEM((WIDE, GROUPS - 1, 2, 2, piece, wide), bf16),
            pltpu.VMEM((WIDE, 2, 2, rows, wide), bf16),
            pltpu.VMEM((n, 2, 2, XS, 2 * rows, wc), bf16),
            pltpu.VMEM((n, 2, rows, wc), bf16),
            pltpu.VMEM((count, width), bf16),
            pltpu.VMEM((2 * count, width), bf16),
            pltpu.VMEM((n, count, wc), bf16),
            dma((WIDE, 2)), dma((WIDE, 2)), dma((WIDE, 2)), dma((1,)),
            dma((WIDE,)), dma((WIDE,)), dma((WIDE,)), dma((WIDE,)),
            dma((WIDE,)), dma((WIDE,)), dma((1,)), dma((1,)),
            dma((n,)), dma((n,)),
            dma((n,)), dma((n,)), dma((n,)), dma((n,)),
            dma((n, 4)), dma((n, 4)),
            dma((n,)), dma((n,)),
        ],
        compiler_params=pltpu.CompilerParams(
            collective_id=0, has_side_effects=True, vmem_limit_bytes=50 * 2**20
        ),
        cost_estimate=pl.CostEstimate(
            flops=4 * count * width * cols, bytes_accessed=2**25, transcendentals=count * cols
        ),
    )(tokens, gain, params, moment, deltas)


def body(tokens, norm_gain, outer_params, momentum, deltas):
    return fused(tokens, norm_gain.reshape(1, -1), outer_params, momentum, deltas[0])


def solution(mesh):
    in_specs = (
        P(("rep", "fsdp"), None),
        P(),
        P(None, "fsdp", None),
        P(None, "fsdp", None),
        P("rep", None, "fsdp", None),
    )
    out_specs = (P(None, "fsdp", None), P(None, "fsdp", None), P(("rep", "fsdp"), None))
    return jax.shard_map(body, mesh=mesh, in_specs=in_specs, out_specs=out_specs, check_vma=False)
```

```python
import functools
import math

import jax
import jax.numpy as jnp
from jax import lax
from jax.experimental import pallas as pl
from jax.experimental.pallas import tpu as pltpu
from jax.sharding import PartitionSpec as P

EPS = 1e-05
MU = 0.9
RATE = 0.7
MESH = pl.DeviceIdType.MESH

CHUNKS = 16
WIDE = CHUNKS // 2
GROUPS = 8
XS = 4
ZS = 4
NORM_STEPS = 4
WAYS = "DYZX"
LAG_Y, LAG_X, LAG_F, LAG_FAR, LAG_P = 4, 6, 8, 10, 12


def kernel(
    tok_ref, gain_ref, p_ref, m_ref, d_ref,
    np_ref, nm_ref, hid_ref,
    dl, rs, sm, w, stg, tk, nt, ob,
    ld_d, ld_p, ld_m, ld_t,
    rs_s, rs_r, sm_s, sm_r, d2_s, d2_r, nt_s, nt_r,
    yo_s, yo_r, x_s, x_r, f_s, f_r, sh_s, sh_r, o_s, o_r,
):
    n = CHUNKS
    rows = dl.shape[3]
    wide = dl.shape[4]
    wc = w.shape[5]
    half = n * wc
    piece = rows // GROUPS
    tokens = tk.shape[0]
    width = tk.shape[1]

    rep = lax.axis_index("rep")
    fs = lax.axis_index("fsdp")
    core = lax.rem(fs, 2)
    other = 1 - core
    chip = fs // 2
    x = lax.rem(chip, XS)
    yh = chip // XS
    yl = lax.rem(rep, 2)
    z = rep // 2
    x_up = lax.rem(x + 1, XS)
    x_dn = lax.rem(x + XS - 1, XS)
    x_far = lax.rem(x + 2, XS)

    def fsdp_of(yh_, x_, core_):
        return (yh_ * XS + x_) * 2 + core_

    partner = (rep, fsdp_of(yh, x, other))
    across = (z * 2 + 1 - yl, fsdp_of(1 - yh, x, core))
    up = (rep, fsdp_of(yh, x_up, core))
    down = (rep, fsdp_of(yh, x_dn, core))
    beside = (z * 2 + 1 - yl, fs)
    layers = [(lax.rem(z + k, ZS) * 2 + yl, fs) for k in (1, 2, 3)]
    peers = [(lax.rem(rep + k, GROUPS), fs) for k in range(1, GROUPS)]

    def wide_columns(jj, h):
        return pl.ds(pl.multiple_of(h * half + jj * wide, wide), wide)

    def load(src, dst, sem, jj, h):
        return pltpu.make_async_copy(
            src.at[:, :, wide_columns(jj, h)], dst.at[jj, h], sem.at[jj, h]
        )

    def load_state(src, dst, sem, jj, h):
        at = wide_columns(jj, h)
        return pltpu.make_async_copy(
            src.at[:, :, at], dst.at[:, :, at], sem.at[jj, h]
        )

    def remote(src, dst, send, recv, device):
        return pltpu.make_async_remote_copy(
            src_ref=src, dst_ref=dst, send_sem=send, recv_sem=recv,
            device_id=device, device_id_type=MESH,
        )

    def rs_copy(jj, k):
        rows_of = pl.multiple_of(peers[k][0] * piece, piece)
        return remote(
            dl.at[jj, :, :, pl.ds(rows_of, piece), :], rs.at[jj, k],
            rs_s.at[jj], rs_r.at[jj], peers[k],
        )

    def sm_copy(jj, k):
        mine = pl.ds(pl.multiple_of(rep * piece, piece), piece)
        ref = sm.at[jj, :, :, mine, :]
        return remote(ref, ref, sm_s.at[jj], sm_r.at[jj], peers[k])

    def d2_copy(jj):
        at = pl.ds(pl.multiple_of(core * rows, rows), rows)
        pair = pl.ds(2 * jj, 2)
        return remote(
            stg.at[pair], w.at[pair, :, yh, x, at, :], d2_s.at[jj], d2_r.at[jj], partner
        )

    def rows_all():
        return pl.ds(0, 2 * rows)

    def rows_half(h):
        return pl.ds(pl.multiple_of(h * rows, rows), rows)

    def rows_quarter():
        size = 2 * rows // ZS
        return pl.ds(pl.multiple_of(z * size, size), size)

    def part(way):
        if way == "Y":
            return rows_half(yl)
        if way == "Z":
            return rows_quarter()
        return rows_all()

    def yo_copy(way, j):
        at = rows_half(1 - yl) if way == "Y" else part(way)
        ref = w.at[j, :, yh, x, at, :]
        return remote(ref, ref, yo_s.at[j], yo_r.at[j], across)

    def x_copy(way, j, k):
        if way == "D":
            ref = w.at[j, :, yh, x]
        else:
            ref = w.at[j, :, :, x, part(way), :]
        return remote(ref, ref, x_s.at[j], x_r.at[j], (up, down)[k])

    def f_copy(way, j, k):
        from_x = (x_dn, x_up)[k]
        if way == "D":
            ref = w.at[j, k, yh, from_x]
        else:
            ref = w.at[j, k, :, from_x, part(way), :]
        return remote(ref, ref, f_s.at[j], f_r.at[j], (up, down)[k])

    def last_legs(way, j, b):
        from_x = (x, x_up, x_dn, x_far)[b]
        if way == "X":
            return []
        if way == "D":
            if b == 0:
                return [yo_copy(way, j)]
            ref = w.at[j, :, yh, from_x]
            return [remote(ref, ref, sh_s.at[j, b], sh_r.at[j, b], across)]
        if b == 0:
            ref = w.at[j, :, 1 - yh, x, part(way), :]
        else:
            ref = w.at[j, :, :, from_x, part(way), :]
        targets = [beside] if way == "Y" else layers
        return [
            remote(ref, ref, sh_s.at[j, b], sh_r.at[j, b], target)
            for k, target in enumerate(targets)
        ]

    def rs_all(jj):
        return remote(rs.at[jj], rs.at[jj], rs_s.at[jj], rs_r.at[jj], partner)

    def sm_all(jj):
        return remote(rs.at[jj], rs.at[jj], sm_s.at[jj], sm_r.at[jj], partner)

    def x_all(way, j):
        if way == "D":
            ref = w.at[j, :, 0, pl.ds(0, 2)]
        else:
            ref = w.at[j, :, :, pl.ds(0, 2), part(way), :]
        return remote(ref, ref, x_s.at[j], x_r.at[j], partner)

    def f_all(way, j):
        if way == "D":
            ref = w.at[j, 0, 0, pl.ds(0, 2)]
        else:
            ref = w.at[j, 0, :, pl.ds(0, 2), part(way), :]
        return remote(ref, ref, f_s.at[j], f_r.at[j], partner)

    def last_all(way, j, b):
        if way != "Z":
            return last_legs(way, j, b)
        if b == 0:
            ref = w.at[j, :, 0, pl.ds(0, 3), part(way), :]
        else:
            ref = w.at[j, :, :, pl.ds(0, 3), part(way), :]
        return [remote(ref, ref, sh_s.at[j, b], sh_r.at[j, b], partner)]

    def share(way, j, b):
        for copy in last_legs(way, j, b):
            copy.start()

    def nt_copy():
        ref = nt.at[pl.ds(pl.multiple_of(core * tokens, tokens), tokens), :]
        return remote(ref, ref, nt_s.at[0], nt_r.at[0], partner)

    def column(j):
        return pl.ds(pl.multiple_of(core * half + j * wc, wc), wc)

    def far_out(j):
        return remote(
            ob.at[j], hid_ref.at[:, column(j)], o_s.at[j], o_r.at[j], partner
        )

    def both(fn):
        for h in range(2):
            fn(h)

    @pl.loop(0, WIDE)
    def _(jj):
        both(lambda h: load(d_ref, dl, ld_d, jj, h).start())

    barrier = pltpu.get_barrier_semaphore()
    friends = peers + [partner, across, up, down]
    for friend in friends:
        pl.semaphore_signal(barrier, inc=1, device_id=friend, device_id_type=MESH)
    pl.semaphore_wait(barrier, len(friends))

    def scatter(jj):
        both(lambda h: load(d_ref, dl, ld_d, jj, h).wait())
        for k in range(GROUPS - 1):
            rs_copy(jj, k).start()

    for jj in range(2):
        scatter(jj)

    pltpu.make_async_copy(tok_ref, tk, ld_t.at[0]).start()

    @pl.loop(0, WIDE)
    def _(jj):
        both(lambda h: load_state(p_ref, np_ref, ld_p, jj, h).start())
        both(lambda h: load_state(m_ref, nm_ref, ld_m, jj, h).start())

    step = 16
    share_of = tokens // NORM_STEPS

    def norm(index):
        if index == 0:
            pltpu.make_async_copy(tok_ref, tk, ld_t.at[0]).wait()

        @pl.loop(0, share_of // step)
        def _(i):
            at = pl.multiple_of(index * share_of + i * step, step)
            values = tk[pl.ds(at, step), :].astype(jnp.float32)
            mean = jnp.sum(values * values, axis=1, keepdims=True) * (1.0 / width)
            scaled = values * lax.rsqrt(mean + EPS) * gain_ref[...]
            base = pl.multiple_of(core * tokens + at, step)
            nt[pl.ds(base, step), :] = scaled.astype(jnp.bfloat16)

    def add_up(jj):
        rs_all(jj).wait_recv()
        mine = pl.ds(pl.multiple_of(rep * piece, piece), piece)
        for h in range(2):
            for q in range(2):
                total = dl[jj, h, q, mine, :].astype(jnp.float32)
                for k in range(GROUPS - 1):
                    total = total + rs[jj, k, h, q].astype(jnp.float32)
                sm[jj, h, q, mine, :] = total.astype(jnp.bfloat16)

    def send_sums(jj):
        for k in range(GROUPS - 1):
            sm_copy(jj, k).start()

    def update(jj):
        sm_all(jj).wait_recv()
        both(lambda h: load_state(p_ref, np_ref, ld_p, jj, h).wait())
        both(lambda h: load_state(m_ref, nm_ref, ld_m, jj, h).wait())
        at = pl.ds(pl.multiple_of(core * rows, rows), rows)

        def weights(h, q):
            grad = sm[jj, h, q].astype(jnp.float32) * (1.0 / GROUPS)
            cols = wide_columns(jj, h)
            moment = MU * nm_ref[q, :, cols] + grad
            fresh = np_ref[q, :, cols] - RATE * (grad + MU * moment)
            nm_ref[q, :, cols] = moment
            np_ref[q, :, cols] = fresh
            return fresh.astype(jnp.bfloat16)

        for q in range(2):
            fresh = weights(other, q)
            for i in range(2):
                stg[2 * jj + i, q] = fresh[:, i * wc:(i + 1) * wc]
        for q in range(2):
            fresh = weights(core, q)
            for i in range(2):
                w[2 * jj + i, q, yh, x, at, :] = fresh[:, i * wc:(i + 1) * wc]

    def hand_over(jj):
        d2_copy(jj).start()

    factor = 1.0 / math.sqrt(width)
    tile = 256

    def project(j):
        def piece_of(base, i):
            left = nt[pl.ds(pl.multiple_of(base * tokens + i * tile, tile), tile), :]
            right = jnp.concatenate(
                [w[j, 0].reshape(width, wc), w[j, 1].reshape(width, wc)], axis=1
            )
            sums = jnp.dot(left, right, preferred_element_type=jnp.float32) * factor
            gate, raised = sums[:, :wc], sums[:, wc:]
            return (gate / (1.0 + jnp.exp(-gate)) * raised).astype(jnp.bfloat16)

        @pl.loop(0, tokens // tile)
        def _(i):
            at = pl.ds(pl.multiple_of(i * tile, tile), tile)
            ob[j, at, :] = piece_of(other, i)

        far_out(j).start()

        @pl.loop(0, tokens // tile)
        def _(i):
            at = pl.ds(pl.multiple_of(i * tile, tile), tile)
            hid_ref[at, column(j)] = piece_of(core, i)

    def stage_y(way, j, first):
        if first:
            d2_copy(j // 2).wait_recv()
        yo_copy(way, j).start()
        if way == "D":
            for k in range(2):
                x_copy(way, j, k).start()

    def stage_x(way, j):
        if way == "D":
            return
        yo_copy(way, j).wait_recv()
        for k in range(2):
            x_copy(way, j, k).start()
        share(way, j, 0)

    def stage_forward(way, j):
        x_all(way, j).wait_recv()
        for k in range(2):
            f_copy(way, j, k).start()
        share(way, j, 1)
        share(way, j, 2)

    def stage_far(way, j):
        f_all(way, j).wait_recv()
        share(way, j, 3)

    def stage_project(way, j):
        for b in range(4):
            for copy in last_all(way, j, b):
                copy.wait_recv()
        project(j)

    cycle = len(WAYS)
    turns = -(-(n + LAG_P) // cycle)

    @pl.loop(0, turns)
    def _(turn):
        for slot in range(cycle):
            t = turn * cycle + slot

            def stage(lag, fn):
                j = t - lag
                way = WAYS[(slot - lag) % cycle]

                @pl.when(jnp.logical_and(j >= 0, j < n))
                def _():
                    fn(way, j)

            def wide_stage(ahead, fn):
                jj = t // 2 + ahead

                @pl.when(jnp.logical_and(jj >= 0, jj < WIDE))
                def _():
                    fn(jj)

            stage(LAG_X, stage_x)
            stage(LAG_Y, lambda way, j: stage_y(way, j, (slot - LAG_Y) % 2 == 0))
            stage(LAG_F, stage_forward)
            stage(LAG_FAR, stage_far)
            if slot % 2 == 1:
                wide_stage(-1, update)
            else:
                wide_stage(0, add_up)
                wide_stage(0, send_sums)
                wide_stage(2, scatter)
            for index in range(NORM_STEPS):
                if index % cycle == slot:

                    @pl.when(t == index)
                    def _():
                        norm(index)

            if NORM_STEPS % cycle == slot:

                @pl.when(t == NORM_STEPS)
                def _():
                    nt_copy().start()

            if slot % 2 == 1:
                wide_stage(-1, hand_over)
            if LAG_P % cycle == slot:

                @pl.when(t == LAG_P)
                def _():
                    nt_copy().wait_recv()

            stage(LAG_P, stage_project)

    nt_copy().wait_send()

    @pl.loop(0, WIDE)
    def _(jj):
        rs_all(jj).wait_send()
        sm_all(jj).wait_send()
        d2_copy(jj).wait_send()

    @pl.loop(0, n // cycle)
    def _(turn):
        for slot, way in enumerate(WAYS):
            j = turn * cycle + slot
            if way != "D":
                yo_copy(way, j).wait_send()
            x_all(way, j).wait_send()
            f_all(way, j).wait_send()
            for b in range(4):
                for copy in last_all(way, j, b):
                    copy.wait_send()
            far_out(j).wait_send()
            far_out(j).wait_recv()


def fused(tokens, gain, params, moment, deltas):
    count, width = tokens.shape
    _, rows, cols = params.shape
    n = CHUNKS
    wc = cols // (2 * n)
    wide = 2 * wc
    piece = rows // GROUPS
    bf16, f32 = jnp.bfloat16, jnp.float32
    dma = pltpu.SemaphoreType.DMA
    any_spec = pl.BlockSpec(memory_space=pl.ANY)
    return pl.pallas_call(
        kernel,
        out_shape=(
            pltpu.VMEM((2, rows, cols), f32),
            pltpu.VMEM((2, rows, cols), f32),
            pltpu.VMEM((count, cols), bf16),
        ),
        in_specs=[any_spec, pl.BlockSpec(memory_space=pltpu.VMEM), any_spec, any_spec, any_spec],
        out_specs=(pl.BlockSpec(memory_space=pltpu.VMEM),) * 3,
        scratch_shapes=[
            pltpu.VMEM((WIDE, 2, 2, rows, wide), bf16),
            pltpu.VMEM((WIDE, GROUPS - 1, 2, 2, piece, wide), bf16),
            pltpu.VMEM((WIDE, 2, 2, rows, wide), bf16),
            pltpu.VMEM((n, 2, 2, XS, 2 * rows, wc), bf16),
            pltpu.VMEM((n, 2, rows, wc), bf16),
            pltpu.VMEM((count, width), bf16),
            pltpu.VMEM((2 * count, width), bf16),
            pltpu.VMEM((n, count, wc), bf16),
            dma((WIDE, 2)), dma((WIDE, 2)), dma((WIDE, 2)), dma((1,)),
            dma((WIDE,)), dma((WIDE,)), dma((WIDE,)), dma((WIDE,)),
            dma((WIDE,)), dma((WIDE,)), dma((1,)), dma((1,)),
            dma((n,)), dma((n,)),
            dma((n,)), dma((n,)), dma((n,)), dma((n,)),
            dma((n, 4)), dma((n, 4)),
            dma((n,)), dma((n,)),
        ],
        compiler_params=pltpu.CompilerParams(
            collective_id=0, has_side_effects=True, vmem_limit_bytes=50 * 2**20
        ),
        cost_estimate=pl.CostEstimate(
            flops=4 * count * width * cols, bytes_accessed=2**25, transcendentals=count * cols
        ),
    )(tokens, gain, params, moment, deltas)


def body(tokens, norm_gain, outer_params, momentum, deltas):
    return fused(tokens, norm_gain.reshape(1, -1), outer_params, momentum, deltas[0])


def solution(mesh):
    in_specs = (
        P(("rep", "fsdp"), None),
        P(),
        P(None, "fsdp", None),
        P(None, "fsdp", None),
        P("rep", None, "fsdp", None),
    )
    out_specs = (P(None, "fsdp", None), P(None, "fsdp", None), P(("rep", "fsdp"), None))
    return jax.shard_map(body, mesh=mesh, in_specs=in_specs, out_specs=out_specs, check_vma=False)
```
